32 devices in a mesh: dp: 4 (over z), vocab: 8 (over y, x, core).
Axes of the slice: x: 2, y: 2, z: 4, core: 2. Of those that a mesh axis runs over, the one named last changes fastest.
Arguments:
- teacher_hidden: bfloat16 [512, 16384], P('vocab', 'dp'), may hold values from -40 to 40
- teacher_weight: bfloat16 [16384, 65536], P('dp', 'vocab'), may hold values from -0.140625 to 0.140625
- student_hidden: bfloat16 [512, 4096], P('vocab', 'dp'), may hold values from -40 to 40
- student_weight: bfloat16 [4096, 65536], P('dp', 'vocab'), may hold values from -0.28125 to 0.28125
Outputs:
- token_kl: float32 [512], P('dp')
- weight_grad: bfloat16 [4096, 65536], P('dp', 'vocab')
The draws below stay inside these ranges and needn't reach their ends.
All inputs are finite; a program needn't handle non-finite values.
Results may differ from the reference program's by a relative error of at most 0.005.
Values may be sent and summed in bfloat16 or wider, within the bound.
No kernel may reach another device: no remote copies, remote signals or barrier semaphores. Data moves between devices by JAX's collectives and lax.ppermute only.
A program may use at most 192 MiB of HBM per device.

```python
import math
import jax
import jax.numpy as jnp

D = 4096
DT = 16384
V = 65536
TOKENS = 512
GRAD_SCALE = 16384


def column_of(weight_key, column, height):
    values = jax.random.normal(jax.random.fold_in(weight_key, column), (height,), jnp.float32)
    values = jnp.clip(values, -6.0, 6.0)
    places = jnp.arange(height)
    values = jnp.where((column == 0) & (places == 0), 6.0, values)
    values = jnp.where((column == 0) & (places == 1), -6.0, values)
    return values * (3.0 / math.sqrt(height))


def whole_weight(key, stream, height):
    weight_key = jax.random.fold_in(key, stream)
    columns = jax.vmap(lambda column: column_of(weight_key, column, height))(jnp.arange(V))
    return columns.T.astype(jnp.bfloat16)


def draw_teacher_weight(key, part):
    return whole_weight(key, 101, DT)


def draw_student_weight(key, part):
    return whole_weight(key, 202, D)


def draw_teacher_hidden(key, part):
    drawn = jax.random.normal(jax.random.fold_in(key, 1), (TOKENS, DT), jnp.float32)
    return jnp.clip(drawn, -6.0, 6.0).astype(jnp.bfloat16)


def draw_student_hidden(key, part):
    drawn = jax.random.normal(jax.random.fold_in(key, 2), (TOKENS, D), jnp.float32)
    return jnp.clip(drawn, -6.0, 6.0).astype(jnp.bfloat16)


def setup_inputs(seed: int = 0) -> dict:
    arg_keys = jax.random.split(jax.random.key(seed), 5)
    teacher_hidden = draw_teacher_hidden(jax.random.fold_in(arg_keys[4], 71), 0)
    teacher_weight = draw_teacher_weight(jax.random.fold_in(arg_keys[4], 71), 0)
    student_hidden = draw_student_hidden(jax.random.fold_in(arg_keys[4], 71), 0)
    student_weight = draw_student_weight(jax.random.fold_in(arg_keys[4], 71), 0)
    return {"teacher_hidden": teacher_hidden, "teacher_weight": teacher_weight, "student_hidden": student_hidden, "student_weight": student_weight}


def reference(teacher_hidden, teacher_weight, student_hidden, student_weight):
    teacher_logits = jnp.dot(teacher_hidden, teacher_weight, preferred_element_type=jnp.float32)
    student_logits = jnp.dot(student_hidden, student_weight, preferred_element_type=jnp.float32)
    teacher_top = jnp.max(teacher_logits, axis=1)
    student_top = jnp.max(student_logits, axis=1)
    teacher_exp = jnp.exp(teacher_logits - teacher_top[:, None])
    teacher_total = jnp.sum(teacher_exp, axis=1)
    numerator = jnp.sum(teacher_exp * (teacher_logits - student_logits), axis=1)
    student_total = jnp.sum(jnp.exp(student_logits - student_top[:, None]), axis=1)
    teacher_lse = teacher_top + jnp.log(teacher_total)
    student_lse = student_top + jnp.log(student_total)
    token_kl = numerator / teacher_total - teacher_lse + student_lse
    factor = GRAD_SCALE / TOKENS
    teacher_prob = jnp.exp(teacher_logits - teacher_lse[:, None])
    student_prob = jnp.exp(student_logits - student_lse[:, None])
    deltas = (factor * (student_prob - teacher_prob)).astype(jnp.bfloat16)
    weight_grad = jnp.dot(student_hidden.T, deltas, preferred_element_type=jnp.float32)
    return token_kl, weight_grad.astype(jnp.bfloat16)
```

```python
import functools

import jax
import jax.numpy as jnp
from jax import lax
from jax.experimental import pallas as pl
from jax.experimental.pallas import tpu as pltpu
from jax.sharding import PartitionSpec as P


LOW = 125.0
SPAN = 250.0
PIECES = 4
VMEM = 48 * 1024 * 1024
F32 = jnp.float32
BF16 = jnp.bfloat16


def call(kernel, operands, in_specs, out_specs, out_shape, grid, name, after=None, scalar=None, aliases=None):
    scalars = [] if scalar is None else [scalar]
    operands = [*scalars, *operands]
    body = kernel
    if after is not None:
        at = len(operands)
        operands.append(after)
        in_specs = [*in_specs, pl.BlockSpec(memory_space=pl.ANY)]
        body = lambda *refs: kernel(*refs[:at], *refs[at + 1 :])
    return pl.pallas_call(
        body,
        grid_spec=pltpu.PrefetchScalarGridSpec(
            num_scalar_prefetch=len(scalars), grid=grid, in_specs=in_specs, out_specs=out_specs
        ),
        out_shape=out_shape,
        input_output_aliases=aliases or {},
        compiler_params=pltpu.CompilerParams(
            dimension_semantics=("arbitrary",) * len(grid), vmem_limit_bytes=VMEM
        ),
        name=name,
    )(*operands)


def product_kernel(hidden_ref, weight_ref, out_ref, top_ref):
    terms = jnp.dot(hidden_ref[...], weight_ref[...], preferred_element_type=F32)
    out_ref[...] = terms
    size = jnp.abs(terms)
    top = size[:, :128]
    for i in range(1, size.shape[1] // 128):
        top = jnp.maximum(top, size[:, i * 128 : (i + 1) * 128])

    @pl.when(pl.program_id(0) == 0)
    def _():
        top_ref[...] = top

    @pl.when(pl.program_id(0) > 0)
    def _():
        top_ref[...] = jnp.maximum(top_ref[...], top)


def partial_logits(hidden, weight, start, width, after=None):
    rows, height = hidden.shape
    block = min(width, 512)
    first = start // block
    return call(
        product_kernel,
        [hidden, weight],
        [
            pl.BlockSpec((rows, height), lambda n: (0, 0)),
            pl.BlockSpec((height, block), lambda n: (0, first + n)),
        ],
        [
            pl.BlockSpec((rows, block), lambda n: (0, n)),
            pl.BlockSpec((rows, 128), lambda n: (0, 0)),
        ],
        [jax.ShapeDtypeStruct((rows, width), F32), jax.ShapeDtypeStruct((rows, 128), F32)],
        (width // block,),
        "partial_logits",
        after,
    )


def decode(code, unit):
    code = code.astype(F32)
    size = (jnp.log2(jnp.abs(code)) + LOW) * unit
    return jnp.where(code < 0, -size, size)


def encode(value, per_unit):
    size = jnp.exp2(jnp.abs(value) * per_unit - LOW)
    return jnp.where(value < 0, -size, size).astype(BF16)


def first_kernel(active_ref, own_ref, top_ref, out_ref):
    @pl.when(active_ref[0] == 1)
    def _():
        out_ref[...] = encode(own_ref[...], SPAN / top_ref[...])


def middle_kernel(active_ref, own_ref, top_ref, code_ref, out_ref):
    @pl.when(active_ref[0] == 1)
    def _():
        top = top_ref[...]
        total = own_ref[...] + decode(code_ref[...], top * (1.0 / SPAN))
        out_ref[...] = encode(total, SPAN / top)


def last_kernel(active_ref, own_ref, top_ref, code_ref, out_ref):
    @pl.when(active_ref[0] == 1)
    def _():
        out_ref[...] = own_ref[...] + decode(code_ref[...], top_ref[...] * (1.0 / SPAN))


def last_stats_kernel(
    active_ref, own_ref, top_ref, code_ref, student_ref, stats_ref, out_ref, new_ref, *, first
):
    @pl.when(active_ref[0] == 1)
    def _():
        teacher = own_ref[...] + decode(code_ref[...], top_ref[...] * (1.0 / SPAN))
        student = student_ref[...]
        out_ref[...] = teacher
        teacher_top = jnp.max(teacher, axis=1, keepdims=True)
        student_top = jnp.max(student, axis=1, keepdims=True)
        if not first:
            stats = stats_ref[...]
            teacher_top = jnp.maximum(teacher_top, stats[:, 0:1])
            student_top = jnp.maximum(student_top, stats[:, 3:4])
        teacher_exp = jnp.exp(teacher - teacher_top)
        teacher_sum = jnp.sum(teacher_exp, axis=1, keepdims=True)
        numerator = jnp.sum(teacher_exp * (teacher - student), axis=1, keepdims=True)
        student_sum = jnp.sum(jnp.exp(student - student_top), axis=1, keepdims=True)
        if not first:
            shrink = jnp.exp(stats[:, 0:1] - teacher_top)
            teacher_sum += shrink * stats[:, 1:2]
            numerator += shrink * stats[:, 2:3]
            student_sum += jnp.exp(stats[:, 3:4] - student_top) * stats[:, 4:5]
        lane = lax.broadcasted_iota(jnp.int32, new_ref.shape, 1)
        new = jnp.where(lane == 0, teacher_top, 0.0)
        new = jnp.where(lane == 1, teacher_sum, new)
        new = jnp.where(lane == 2, numerator, new)
        new = jnp.where(lane == 3, student_top, new)
        new_ref[...] = jnp.where(lane == 4, student_sum, new)


def step(kernel, active, own, half, top, after, code=None, student=None, stats=None):
    own, piece, width = own
    rows = own.shape[0] // 2
    tile = min(rows, 64)
    tiles = rows // tile
    operands = [own, top]
    plain = pl.BlockSpec((tile, width), lambda i, a: (i * a[0], 0))
    in_specs = [
        pl.BlockSpec((tile, width), lambda i, a: (half * tiles + i * a[0], piece)),
        pl.BlockSpec((tile, 1), lambda i, a: (half * tiles + i * a[0], 0)),
    ]
    if code is not None:
        operands.append(code)
        in_specs.append(plain)
    final = kernel in (last_kernel, last_stats_kernel)
    out_shape = jax.ShapeDtypeStruct((rows, width), F32 if final else BF16)
    out_specs = plain
    if kernel is last_stats_kernel:
        first = stats is None
        lanes = pl.BlockSpec((tile, 128), lambda i, a: (i * a[0], 0))
        stats = jnp.zeros((rows, 128), F32) if first else stats
        operands += [student, stats]
        in_specs += [plain, lanes]
        out_shape = [out_shape, jax.ShapeDtypeStruct((rows, 128), F32)]
        out_specs = [plain, lanes]
        kernel = functools.partial(kernel, first=first)
    return call(kernel, operands, in_specs, out_specs, out_shape, (tiles,), "chain_step", after, active)


def in_turn(value, after):
    return call(
        lambda *refs: None,
        [value],
        [pl.BlockSpec(memory_space=pl.ANY)],
        pl.BlockSpec(memory_space=pl.ANY),
        jax.ShapeDtypeStruct(value.shape, value.dtype),
        (1,),
        "in_turn",
        after,
        aliases={0: 0},
    )


def delta_kernel(active_ref, teacher_ref, student_ref, lse_ref, out_ref, *, factor):
    @pl.when(active_ref[0] == 1)
    def _():
        lse = lse_ref[...]
        teacher_prob = jnp.exp(teacher_ref[...] - lse[:, 0:1])
        student_prob = jnp.exp(student_ref[...] - lse[:, 1:2])
        out_ref[...] = (factor * (student_prob - teacher_prob)).astype(BF16)


def delta_piece(active, teacher, student, lse, factor, after):
    rows, width = teacher.shape
    tile = min(rows, 64)
    plain = pl.BlockSpec((tile, width), lambda i, a: (i * a[0], 0))
    return call(
        functools.partial(delta_kernel, factor=factor),
        [teacher, student, lse],
        [plain, plain, pl.BlockSpec((tile, 2), lambda i, a: (i * a[0], 0))],
        plain,
        jax.ShapeDtypeStruct((rows, width), BF16),
        (rows // tile,),
        "delta_piece",
        after,
        active,
    )


def grad_kernel(place_ref, hidden_ref, *refs):
    arrived, out_ref = refs[:-1], refs[-1]
    place = place_ref[0]
    hops = len(arrived)
    near, far = arrived[0][...], arrived[hops - 1][...]
    for k in range(1, hops // 2):
        near = jnp.where(place == k, arrived[k][...], near)
        far = jnp.where(place == k, arrived[hops - 1 - k][...], far)
    half = near.shape[0]
    product = functools.partial(
        lax.dot_general,
        dimension_numbers=(((0,), (0,)), ((), ())),
        preferred_element_type=F32,
    )
    out_ref[...] = (product(hidden_ref[:half], far) + product(hidden_ref[half:], near)).astype(BF16)


def grad_piece(place, hidden, arrived, piece, total, out, after):
    rows, high = hidden.shape
    half, width = arrived[0].shape
    tile = min(high, 256)
    in_specs = [pl.BlockSpec((rows, tile), lambda i, p: (0, i))]
    in_specs += [pl.BlockSpec((half, width), lambda i, p: (0, 0)) for _ in arrived]
    operands = [hidden, *arrived]
    kernel, aliases = grad_kernel, {}
    if out is not None:
        in_specs.append(pl.BlockSpec(memory_space=pl.ANY))
        operands.append(out)
        aliases = {len(operands): 0}
        kernel = lambda *refs: grad_kernel(*refs[:-2], refs[-1])
    return call(
        kernel,
        operands,
        in_specs,
        pl.BlockSpec((tile, width), lambda i, p: (i, piece)),
        jax.ShapeDtypeStruct((high, total), BF16),
        (high // tile,),
        "grad_piece",
        after,
        place,
        aliases,
    )


def swap(value, axis, mask):
    return lax.ppermute(value, axis, [(i, i ^ mask) for i in range(lax.axis_size(axis))])


def gather_rows(hidden, near_first):
    count = lax.axis_size("vocab")
    mine = [hidden] + [swap(hidden, "vocab", mask) for mask in range(2, count, 2)]
    half = len(mine) // 2
    low, high = jnp.concatenate(mine[:half]), jnp.concatenate(mine[half:])
    parts = jnp.concatenate([low, swap(low, "vocab", 1), high, swap(high, "vocab", 1)])
    rows = parts.shape[0] // 2
    return jnp.where(near_first, jnp.concatenate([parts[rows:], parts[:rows]]), parts)


def half_masks(count):
    return [m for m in range(0, count // 2, 2)] + [m + 1 for m in range(0, count // 2, 2)]


def shared_top(tops):
    total = jnp.max(functools.reduce(jnp.maximum, tops), axis=1)
    deep = lax.axis_size("dp")
    mask = 1
    while mask < deep:
        other = swap(total, "dp", mask)
        total = total + (jnp.roll(other, total.shape[0] // 2) if 2 * mask == deep else other)
        mask *= 2
    return jnp.maximum(total * 1.001, 1e-30)[:, None]


def body(teacher_hidden, teacher_weight, student_hidden, student_weight):
    deep = lax.axis_size("dp")
    vocab_count = lax.axis_size("vocab")
    z, v = lax.axis_index("dp"), lax.axis_index("vocab")
    columns = teacher_weight.shape[1]
    width = columns // PIECES
    place = jnp.minimum(z, deep - 1 - z)
    upper = (z >= deep // 2).astype(jnp.int32)
    top_bit = (v >= vocab_count // 2).astype(jnp.int32)
    near_first = upper == top_bit
    place_array = jnp.reshape(place, (1,)).astype(jnp.int32)
    active = [
        jnp.reshape(place == min(k, deep - 1 - k), (1,)).astype(jnp.int32) for k in range(deep)
    ]
    hops = [[(k - 1, k), (deep - k, deep - 1 - k)] for k in range(1, deep)]

    student_rows = gather_rows(student_hidden, near_first)
    teacher_rows = gather_rows(teacher_hidden, near_first)
    tokens = student_rows.shape[0]
    half_rows = tokens // 2

    logits, top = partial_logits(student_rows, student_weight, 0, columns)
    student_top = shared_top([top])
    after = logits
    own = [(logits, c, width) for c in range(PIECES)] + [None] * PIECES
    tops = [student_top] * PIECES + [None] * PIECES
    teacher_tops = []

    moving, final, stats = [None] * (2 * PIECES), [None] * (2 * PIECES), None
    for tick in range(2 * PIECES + deep - 1):
        for k in range(deep):
            c = tick - k
            if not 0 <= c < 2 * PIECES:
                continue
            half = int(k >= deep // 2)
            turn = (active[k], own[c], half, tops[c], after)
            if k == 0:
                code = after = step(first_kernel, *turn)
            elif k < deep - 1:
                code = after = step(middle_kernel, *turn, moving[c])
            elif c < PIECES:
                final[c] = after = step(last_kernel, *turn, moving[c])
            else:
                final[c], stats = step(
                    last_stats_kernel, *turn, moving[c], student=final[c - PIECES], stats=stats
                )
                after = stats
            if k < deep - 1:
                moving[c] = lax.ppermute(code, "dp", hops[k])
            if k == 0 and c < PIECES:
                logits, top = partial_logits(teacher_rows, teacher_weight, c * width, width, after)
                after = top
                own[PIECES + c] = (logits, 0, width)
                teacher_tops.append(top)
                if c == PIECES - 1:
                    tops[PIECES:] = [shared_top(teacher_tops)] * PIECES
    student, teacher = final[:PIECES], final[PIECES:]

    masks = half_masks(vocab_count)
    block = half_rows // len(masks)
    sums = stats[:, :5].T.reshape(5, len(masks), block)
    mask = 1
    while mask < vocab_count:
        other = swap(sums, "vocab", mask)
        low = mask % (vocab_count // 2)
        other = jnp.stack([other[:, masks.index(m ^ low)] for m in masks], axis=1)
        top_t, top_s = jnp.maximum(sums[0], other[0]), jnp.maximum(sums[3], other[3])
        ours_t, theirs_t = jnp.exp(sums[0] - top_t), jnp.exp(other[0] - top_t)
        ours_s, theirs_s = jnp.exp(sums[3] - top_s), jnp.exp(other[3] - top_s)
        sums = jnp.stack(
            [
                top_t,
                sums[1] * ours_t + other[1] * theirs_t,
                sums[2] * ours_t + other[2] * theirs_t,
                top_s,
                sums[4] * ours_s + other[4] * theirs_s,
            ]
        )
        mask *= 2
    teacher_lse = sums[0] + jnp.log(sums[1])
    student_lse = sums[3] + jnp.log(sums[4])
    token_kl = sums[2] / sums[1] - teacher_lse + student_lse
    lse = jnp.stack([teacher_lse.reshape(-1), student_lse.reshape(-1)], axis=1)

    factor = float(columns * vocab_count // 4 / tokens)
    grad, arrived = None, [[] for _ in range(PIECES)]
    after = lse
    for tick in range(PIECES + deep - 1):
        for k in range(deep):
            c = tick - k
            if not 0 <= c < PIECES:
                continue
            if k == 0:
                after = delta_piece(active[0], teacher[c], student[c], lse, factor, after)
                arrived[c].append(after)
            elif k < deep - 1:
                after = in_turn(moving[c], after)
                arrived[c].append(after)
            else:
                arrived[c].append(moving[c])
                grad = after = grad_piece(
                    place_array, student_rows, arrived[c], c, columns, grad, after if grad is None else None
                )
            if k < deep - 1:
                moving[c] = lax.ppermute(after, "dp", hops[k])

    low = v % (vocab_count // 2)
    source = jnp.array(masks)[None, :] ^ low
    ordered = jnp.sum(
        jnp.where(
            (source == jnp.arange(len(masks))[:, None])[:, :, None], token_kl[None], 0.0
        ),
        axis=1,
    ).reshape(deep // 2, -1)
    ordered = jnp.where(upper == 1, ordered[::-1], ordered)
    share = jnp.where(place == 0, ordered[0], 0.0)
    for k in range(1, deep // 2):
        share = share + lax.ppermute(ordered[k], "dp", [(0, k), (deep - 1, deep - 1 - k)])
    return share, grad


def solution(mesh):
    placed = (P("vocab", "dp"), P("dp", "vocab"), P("vocab", "dp"), P("dp", "vocab"))
    return jax.shard_map(
        body, mesh=mesh, in_specs=placed, out_specs=(P("dp"), P("dp", "vocab")), check_vma=False
    )
```
